32 devices in a mesh: band: 8 (over y, x, core), field: 4 (over z).
Axes of the slice: x: 2, y: 2, z: 4, core: 2. Of those that a mesh axis runs over, the one named last changes fastest.
Arguments:
- fourier: bfloat16 [32, 192, 448], P(None, 'field', 'band'), may hold values from -6 to 6
- quad_weights: float32 [448], P('band'), may hold values from 0.1 to 1.9
- legendre: bfloat16 [32, 448, 32], P(('band', 'field')), may hold values from -0.25 to 0.25
- slot_wave: int32 [32], replicated, may hold values from 0 to 31, each once
- vert_proj: float32 [96, 96], replicated, may hold values from -0.625 to 0.625
- vert_recon: float32 [96, 96], replicated, may hold values from -0.625 to 0.625
- vert_rates: float32 [96], replicated, may hold values from 0.3 to 30
Outputs:
- spectral: bfloat16 [32, 2, 96, 32], P(('band', 'field'))
- returned: bfloat16 [32, 192, 448], P(None, 'field', 'band')
The draws below stay inside these ranges and needn't reach their ends.
Inputs may be any that keep to these rules, and one draw needn't show every extreme that they name: `slot_wave`: every wavenumber 0 .. 31 stands in exactly one slot.
All inputs are finite; a program needn't handle non-finite values.
Results may differ from the reference program's by a relative error of at most 0.0056.
Values may be sent and summed in bfloat16 or wider, within the bound.
A program may use at most 64 MiB of HBM per device.

```python
import math
import jax
import jax.numpy as jnp
from jax import lax

LEV = 96
T_SIZE = 32
NLAT = 448


def block_scale(key, extent, cuts, least, top_value):
    def one(dim, parts):
        heights = jax.random.uniform(jax.random.fold_in(jax.random.fold_in(key, 6), dim), (parts,), jnp.float32, least / len(cuts), top_value / len(cuts))
        return jnp.repeat(jnp.exp(heights), extent[dim] // parts).reshape((-1,) + (1,) * (len(extent) - dim - 1))

    factor_of = one(*cuts[0])
    for cut in cuts[1:]:
        factor_of = factor_of * one(*cut)
    return factor_of


def bell_draw(own_key, dims, deviation, reach, cuts=(), held_as=jnp.bfloat16):
    loudness = block_scale(own_key, dims, cuts, -0.22, 0.18) if cuts else 1.0
    drawn = jax.random.normal(own_key, dims, jnp.float32) * deviation * loudness
    return jnp.minimum(jnp.maximum(drawn, -reach), reach).astype(held_as)


def setup_inputs(seed: int = 0) -> dict:
    splits = jax.random.split(jax.random.key(seed), 8)
    fourier = bell_draw(splits[0], (T_SIZE, 2 * LEV, NLAT), 1.0, 6.0, ((1, 4), (2, 8)))
    quad_weights = jnp.clip(1.0 + 0.18 * jax.random.normal(splits[1], (NLAT,), jnp.float32), 0.1, 1.9)
    legendre = bell_draw(splits[2], (T_SIZE, NLAT, T_SIZE), NLAT ** -0.5, 0.25, ((0, 32),))
    slot_wave = jax.random.permutation(splits[3], T_SIZE).astype(jnp.int32)
    vert_proj = bell_draw(splits[4], (LEV, LEV), LEV ** -0.5, 0.625, (), jnp.float32)
    vert_recon = bell_draw(splits[5], (LEV, LEV), LEV ** -0.5, 0.625, (), jnp.float32)
    vert_rates = jnp.clip(jnp.exp(jax.random.uniform(splits[6], (LEV,), jnp.float32, math.log(0.3), math.log(30.0))), 0.3, 30.0)
    return dict(fourier=fourier, quad_weights=quad_weights, legendre=legendre, slot_wave=slot_wave, vert_proj=vert_proj, vert_recon=vert_recon, vert_rates=vert_rates)


def damping(vert_rates, total):
    order = jnp.arange(total).astype(jnp.float32)
    growth = order * (order + 1.0) / float(total * total)
    return 1.0 / (1.0 + vert_rates[:, None] * growth[None, :])


def reference(fourier, quad_weights, legendre, slot_wave, vert_proj, vert_recon, vert_rates):
    weighted = (fourier.astype(jnp.float32) * quad_weights).astype(jnp.bfloat16)
    gamma = damping(vert_rates, T_SIZE)
    degree = jnp.arange(T_SIZE).astype(jnp.int32)

    def one_slot(items):
        table, wave = items
        data = weighted[wave]
        direct = jnp.dot(data, table, preferred_element_type=jnp.float32).reshape(2, LEV, T_SIZE)
        modes = jnp.einsum("jl,cln->cjn", vert_proj, direct, precision=lax.Precision.HIGHEST) * gamma
        solved = jnp.einsum("lj,cjn->cln", vert_recon, modes, precision=lax.Precision.HIGHEST)
        keep = (degree >= wave).astype(jnp.float32)
        spectral_one = (solved * keep).astype(jnp.bfloat16)
        back = lax.dot_general(spectral_one.reshape(2 * LEV, T_SIZE), table, (((1,), (1,)), ((), ())),
                               preferred_element_type=jnp.float32)
        return spectral_one, back.astype(jnp.bfloat16)

    spectral, backs = lax.map(one_slot, (legendre, slot_wave.astype(jnp.int32)))
    inverse = jnp.zeros((T_SIZE,), jnp.int32).at[slot_wave].set(jnp.arange(T_SIZE).astype(jnp.int32))
    return spectral, backs[inverse]
```

```python
import functools

import jax
import jax.numpy as jnp
from jax import lax
from jax.experimental import pallas as pl
from jax.experimental.pallas import tpu as pltpu
from jax.sharding import PartitionSpec as P

LEV = 96
LANES = 128
MESH = pl.DeviceIdType.MESH


def exchange(
    nb, nf, pack, wave_ref, quad_ref, rates_ref, leg_ref, proj_ref, recon_ref, fourier_ref,
    spec_ref, back_ref,
    four_v, send_a, recv_a, send_b, table, acc, four_sem, send_a_sem, recv_a_sem, send_b_sem, recv_b_sem,
):
    n_dev = nb * nf
    my_b, my_f = lax.axis_index("band"), lax.axis_index("field")
    me = my_b * nf + my_f
    rows, width = fourier_ref.shape[1], fourier_ref.shape[2]
    part = rows // pack
    total = leg_ref.shape[2]

    def peer(step):
        other = lax.rem(me + step, n_dev)
        return other, (other // nf, lax.rem(other, nf))

    fetch = pltpu.make_async_copy(fourier_ref, four_v, four_sem)
    fetch.start()
    barrier = pltpu.get_barrier_semaphore()

    @pl.loop(1, n_dev)
    def _(step):
        pl.semaphore_signal(barrier, inc=1, device_id=peer(step)[1], device_id_type=MESH)

    @pl.loop(0, nb)
    def _(b):
        block = leg_ref[0, pl.ds(pl.multiple_of(b * width, 8), width), :].astype(jnp.float32)
        pieces = []
        for h in range(pack):
            line = [jnp.zeros((width, total), jnp.float32)] * pack
            line[h] = block
            pieces.append(jnp.concatenate(line, axis=1) if pack > 1 else block)
        pieces.append(jnp.zeros((LANES - pack * width, pack * total), jnp.float32))
        table[b] = jnp.concatenate(pieces, axis=0).astype(jnp.bfloat16)

    fetch.wait()
    quad = quad_ref[...]

    @pl.loop(0, n_dev)
    def _(s):
        x = (four_v[wave_ref[s]].astype(jnp.float32) * quad)
        pieces = [x[h * part : (h + 1) * part] for h in range(pack)]
        pieces.append(jnp.zeros((part, LANES - pack * width), jnp.float32))
        send_a[s] = jnp.concatenate(pieces, axis=1).astype(jnp.bfloat16)

    pl.semaphore_wait(barrier, n_dev - 1)

    own_a = pltpu.make_async_copy(send_a.at[me], recv_a.at[my_b, my_f], recv_a_sem.at[my_b])
    own_a.start()

    @pl.loop(1, n_dev)
    def _(step):
        other, where = peer(step)
        pltpu.make_async_remote_copy(
            src_ref=send_a.at[other],
            dst_ref=recv_a.at[my_b, my_f],
            send_sem=send_a_sem,
            recv_sem=recv_a_sem.at[my_b],
            device_id=where,
            device_id_type=MESH,
        ).start()

    eye = lax.broadcasted_iota(jnp.int32, (LEV, LEV), 0) == lax.broadcasted_iota(jnp.int32, (LEV, LEV), 1)
    rates = jnp.sum(jnp.where(eye, rates_ref[...], 0.0), axis=1, keepdims=True)
    degree = lax.broadcasted_iota(jnp.int32, (1, 2 * total), 1)
    degree = jnp.where(degree >= total, degree - total, degree)
    order = degree.astype(jnp.float32)
    gamma = 1.0 / (1.0 + rates * (order * (order + 1.0) / float(total * total)))
    keep = (degree >= wave_ref[me]).astype(jnp.float32)

    acc[...] = jnp.zeros_like(acc)

    @pl.loop(0, nb)
    def _(step):
        b = lax.rem(my_b + step, nb)
        pltpu.make_async_copy(recv_a.at[b], recv_a.at[b], recv_a_sem.at[b]).wait()
        data = recv_a[b].reshape(nf * part, LANES)
        acc[...] += jnp.dot(data, table[b], preferred_element_type=jnp.float32)

    per_c = nf * pack // 2
    group = [acc[(g // pack) * part : (g // pack + 1) * part, (g % pack) * total : (g % pack + 1) * total]
             for g in range(nf * pack)]
    direct = jnp.concatenate(
        [jnp.concatenate(group[c * per_c : (c + 1) * per_c], axis=0) for c in range(2)], axis=1
    )
    exact = dict(preferred_element_type=jnp.float32, precision=lax.Precision.HIGHEST)
    modes = jnp.dot(proj_ref[...], direct, **exact) * gamma
    solved = jnp.dot(recon_ref[...], modes, **exact) * keep
    for c in range(2):
        spec_ref[c] = solved[:, c * total : (c + 1) * total].astype(jnp.bfloat16)

    def piece(g):
        c, l = g // per_c, (g % per_c) * part
        return solved[l : l + part, c * total : (c + 1) * total]

    packed = jnp.concatenate(
        [jnp.concatenate([piece(f * pack + h) for h in range(pack)], axis=1) for f in range(nf)], axis=0
    ).astype(jnp.bfloat16)

    @pl.loop(0, nb)
    def _(b):
        out = lax.dot_general(packed, table[b], (((1,), (1,)), ((), ())), preferred_element_type=jnp.float32)
        send_b[pl.ds(b * nf, nf)] = out.astype(jnp.bfloat16).reshape(nf, part, LANES)

    own_b = pltpu.make_async_copy(send_b.at[me], back_ref.at[me], recv_b_sem)
    own_b.start()

    @pl.loop(1, n_dev)
    def _(step):
        other, where = peer(step)
        pltpu.make_async_remote_copy(
            src_ref=send_b.at[other],
            dst_ref=back_ref.at[me],
            send_sem=send_b_sem,
            recv_sem=recv_b_sem,
            device_id=where,
            device_id_type=MESH,
        ).start()

    pltpu.make_async_copy(back_ref, back_ref, recv_b_sem).wait()
    others = pl.ds(0, n_dev - 1)
    pltpu.make_async_copy(send_a.at[others], send_a.at[others], send_a_sem).wait()
    pltpu.make_async_copy(send_b.at[others], send_b.at[others], send_b_sem).wait()


def unpack(pack, wave_ref, back_ref, spec_in, spec_out, out_ref):
    part = back_ref.shape[1]
    width = out_ref.shape[2]
    spec_out[0] = spec_in[...]

    @pl.loop(0, back_ref.shape[0])
    def _(s):
        w = wave_ref[s]
        x = back_ref[s].astype(jnp.float32)
        for h in range(pack):
            out_ref[w, h * part : (h + 1) * part, :] = x[:, h * width : (h + 1) * width].astype(jnp.bfloat16)


def per_device(fourier, quad_weights, legendre, slot_wave, vert_proj, vert_recon, vert_rates):
    nb, nf = lax.axis_size("band"), lax.axis_size("field")
    n_dev = nb * nf
    waves, rows, width = fourier.shape
    per_dev, nlat, total = legendre.shape
    assert per_dev == 1 and waves == n_dev and nlat == nb * width and width <= LANES
    pack = 1
    while rows % (2 * pack * 8) == 0 and 2 * pack * width <= LANES and 2 * pack * total <= LANES:
        pack *= 2
    part = rows // pack
    vmem = pl.BlockSpec(memory_space=pltpu.VMEM)
    smem = pl.BlockSpec(memory_space=pltpu.SMEM)
    anywhere = pl.BlockSpec(memory_space=pl.ANY)
    blocks = (n_dev, part, LANES)
    spec, back = pl.pallas_call(
        functools.partial(exchange, nb, nf, pack),
        out_shape=(
            jax.ShapeDtypeStruct((2, LEV, total), jnp.bfloat16),
            jax.ShapeDtypeStruct(blocks, jnp.bfloat16),
        ),
        in_specs=[smem, vmem, vmem, vmem, vmem, vmem, anywhere],
        out_specs=(vmem, vmem),
        scratch_shapes=[
            pltpu.VMEM(fourier.shape, jnp.bfloat16),
            pltpu.VMEM(blocks, jnp.bfloat16),
            pltpu.VMEM((nb, nf, part, LANES), jnp.bfloat16),
            pltpu.VMEM(blocks, jnp.bfloat16),
            pltpu.VMEM((nb, LANES, pack * total), jnp.bfloat16),
            pltpu.VMEM((nf * part, pack * total), jnp.float32),
            pltpu.SemaphoreType.DMA,
            pltpu.SemaphoreType.DMA,
            pltpu.SemaphoreType.DMA((nb,)),
            pltpu.SemaphoreType.DMA,
            pltpu.SemaphoreType.DMA,
        ],
        compiler_params=pltpu.CompilerParams(collective_id=0, has_side_effects=True),
    )(slot_wave, quad_weights[None], vert_rates[None], legendre, vert_proj, vert_recon, fourier)
    spectral, returned = pl.pallas_call(
        functools.partial(unpack, pack),
        out_shape=(
            jax.ShapeDtypeStruct((1, 2, LEV, total), jnp.bfloat16),
            jax.ShapeDtypeStruct(fourier.shape, jnp.bfloat16),
        ),
        in_specs=[smem, vmem, vmem],
        out_specs=(vmem, vmem),
    )(slot_wave, back, spec)
    return spectral, returned


def solution(mesh):
    placed = (
        P(None, "field", "band"),
        P("band"),
        P(("band", "field"), None, None),
        P(),
        P(),
        P(),
        P(),
    )
    return jax.shard_map(
        per_device,
        mesh=mesh,
        in_specs=placed,
        out_specs=(P(("band", "field"), None, None, None), P(None, "field", "band")),
        check_vma=False,
    )
```

```python
import functools

import jax
import jax.numpy as jnp
from jax import lax
from jax.experimental import pallas as pl
from jax.experimental.pallas import tpu as pltpu
from jax.sharding import PartitionSpec as P

LEV = 96
LANES = 128
UNROLL = 4
CHUNKS = 4
VMEM_LIMIT = 60 * 1024 * 1024
MESH = pl.DeviceIdType.MESH


def exchange(
    nb, nf, pack, wave_hbm, row_hbm, quad_hbm, rates_hbm, leg_hbm, proj_hbm, recon_hbm, fourier_hbm,
    spec_ref, out_ref,
    wave, order, row, quad, rates, leg, proj, recon, four, send_a, recv_a, send_b, recv_b, table, acc,
    inverse_v, spec_v, out_v,
    small_sem, four_sem, out_sem, send_a_sem, recv_a_sem, send_b_sem, recv_b_sem,
):
    n_dev = nb * nf
    my_b, my_f = lax.axis_index("band"), lax.axis_index("field")
    me = my_b * nf + my_f
    rows, width = four.shape[1], four.shape[2]
    part = rows // pack
    total = leg.shape[1]

    def peer(step):
        other = lax.rem(me + step, n_dev)
        return other, (other // nf, lax.rem(other, nf))

    barrier = pltpu.get_barrier_semaphore()

    @pl.loop(1, n_dev, unroll=UNROLL)
    def _(step):
        pl.semaphore_signal(barrier, inc=1, device_id=peer(step)[1], device_id_type=MESH)

    pairs = ((wave_hbm, wave), (quad_hbm, quad), (row_hbm, row), (leg_hbm, leg), (rates_hbm, rates),
             (proj_hbm, proj), (recon_hbm, recon))
    loads = [pltpu.make_async_copy(a, b, small_sem.at[i]) for i, (a, b) in enumerate(pairs)]
    fetch = pltpu.make_async_copy(fourier_hbm, four, four_sem)
    loads[0].start()
    loads[1].start()
    fetch.start()
    for load in loads[2:]:
        load.start()
    loads[0].wait()
    loads[1].wait()
    fetch.wait()

    @pl.loop(0, n_dev, unroll=UNROLL)
    def _(s):
        x = four[jnp.clip(wave[s], 0, n_dev - 1)].astype(jnp.float32) * quad[...]
        pieces = [x[h * part : (h + 1) * part] for h in range(pack)]
        pieces.append(jnp.zeros((part, LANES - pack * width), jnp.float32))
        send_a[s] = jnp.concatenate(pieces, axis=1).astype(jnp.bfloat16)

    pl.semaphore_wait(barrier, n_dev - 1)

    @pl.loop(1, n_dev, unroll=UNROLL)
    def _(step):
        other, where = peer(step)
        pltpu.make_async_remote_copy(
            src_ref=send_a.at[other],
            dst_ref=recv_a.at[my_b, my_f],
            send_sem=send_a_sem,
            recv_sem=recv_a_sem.at[my_b],
            device_id=where,
            device_id_type=MESH,
        ).start()

    pltpu.make_async_copy(send_a.at[me], recv_a.at[my_b, my_f], recv_a_sem.at[my_b]).start()

    loads[2].wait()
    down = lax.broadcasted_iota(jnp.int32, (n_dev, n_dev), 0)
    across = lax.broadcasted_iota(jnp.int32, (n_dev, n_dev), 1)
    aim = lax.broadcasted_iota(jnp.int32, (n_dev, inverse_v.shape[1]), 1)
    source = lax.broadcasted_iota(jnp.int32, (n_dev, inverse_v.shape[1]), 0)
    column = jnp.sum(jnp.where(down == across, row[...].astype(jnp.float32), 0.0), axis=1, keepdims=True)
    hit = column.astype(jnp.int32) == aim
    inverse_v[...] = jnp.sum(jnp.where(hit, source.astype(jnp.float32), 0.0), axis=0, keepdims=True).astype(jnp.int32)

    loads[3].wait()
    for b in range(nb):
        block = leg[0, :, b * width : (b + 1) * width].astype(jnp.float32)
        lines = []
        for h in range(pack):
            line = [jnp.zeros((total, h * width), jnp.float32)] if h else []
            line += [block, jnp.zeros((total, LANES - (h + 1) * width), jnp.float32)]
            lines.append(jnp.concatenate(line, axis=1))
        table[b] = jnp.concatenate(lines, axis=0).astype(jnp.bfloat16)

    to_scalar = pltpu.make_async_copy(inverse_v, order, small_sem.at[2])
    to_scalar.start()
    for load in loads[4:]:
        load.wait()
    degree = lax.broadcasted_iota(jnp.int32, (2 * total, 1), 0)
    degree = jnp.where(degree >= total, degree - total, degree)
    level = degree.astype(jnp.float32)
    gamma = 1.0 / (1.0 + rates[...] * (level * (level + 1.0) / float(total * total)))
    keep = (degree >= wave[me]).astype(jnp.float32)
    to_scalar.wait()

    acc[...] = jnp.zeros_like(acc)

    across_rows = (((1,), (1,)), ((), ()))

    @pl.loop(0, nb)
    def _(step):
        b = lax.rem(my_b + step, nb)
        pltpu.make_async_copy(recv_a.at[b], recv_a.at[b], recv_a_sem.at[b]).wait()
        data = recv_a[b].reshape(nf * part, LANES)
        acc[...] += lax.dot_general(table[b], data, across_rows, preferred_element_type=jnp.float32)

    per_c = nf * pack // 2
    group = [acc[(g % pack) * total : (g % pack + 1) * total, (g // pack) * part : (g // pack + 1) * part]
             for g in range(nf * pack)]
    direct = jnp.concatenate(
        [jnp.concatenate(group[c * per_c : (c + 1) * per_c], axis=1) for c in range(2)], axis=0
    )
    exact = dict(preferred_element_type=jnp.float32, precision=lax.Precision.HIGHEST)
    modes = lax.dot_general(direct, proj[...], across_rows, **exact) * gamma
    solved = lax.dot_general(modes, recon[...], across_rows, **exact) * keep

    def piece(g):
        c, l = g // per_c, (g % per_c) * part
        return solved[c * total : (c + 1) * total, l : l + part]

    packed = jnp.concatenate(
        [jnp.concatenate([piece(f * pack + h) for f in range(nf)], axis=1) for h in range(pack)], axis=0
    ).T.astype(jnp.bfloat16)

    @pl.loop(0, nb, unroll=UNROLL)
    def _(b):
        got = jnp.dot(packed, table[b], preferred_element_type=jnp.float32)
        send_b[pl.ds(b * nf, nf)] = got.astype(jnp.bfloat16).reshape(nf, part, LANES)

    @pl.loop(1, n_dev, unroll=UNROLL)
    def _(step):
        other, where = peer(step)
        pltpu.make_async_remote_copy(
            src_ref=send_b.at[other],
            dst_ref=recv_b.at[me],
            send_sem=send_b_sem,
            recv_sem=recv_b_sem,
            device_id=where,
            device_id_type=MESH,
        ).start()

    pltpu.make_async_copy(send_b.at[me], recv_b.at[me], recv_b_sem).start()
    spec_v[...] = solved.astype(jnp.bfloat16).reshape(1, 2, total, LEV)
    spec_out = pltpu.make_async_copy(spec_v, spec_ref, small_sem.at[0])
    spec_out.start()
    pltpu.make_async_copy(recv_b, recv_b, recv_b_sem).wait()

    size = n_dev // CHUNKS
    outs = []
    for k in range(CHUNKS):
        @pl.loop(k * size, (k + 1) * size, unroll=UNROLL)
        def _(w):
            x = recv_b[jnp.clip(order[0, w], 0, n_dev - 1)].astype(jnp.float32)
            for h in range(pack):
                out_v[w, h * part : (h + 1) * part, :] = x[:, h * width : (h + 1) * width].astype(jnp.bfloat16)
        span = pl.ds(k * size, size)
        outs.append(pltpu.make_async_copy(out_v.at[span], out_ref.at[span], out_sem.at[k]))
        outs[-1].start()

    spec_out.wait()
    others = pl.ds(0, n_dev - 1)
    pltpu.make_async_copy(send_a.at[others], send_a.at[others], send_a_sem).wait()
    pltpu.make_async_copy(send_b.at[others], send_b.at[others], send_b_sem).wait()
    for out in outs:
        out.wait()


def per_device(fourier, quad_weights, legendre, slot_wave, vert_proj, vert_recon, vert_rates):
    nb, nf = lax.axis_size("band"), lax.axis_size("field")
    n_dev = nb * nf
    waves, rows, width = fourier.shape
    per_dev, nlat, total = legendre.shape
    assert per_dev == 1 and waves == n_dev and nlat == nb * width and width <= LANES
    pack = 1
    while rows % (2 * pack * 8) == 0 and 2 * pack * width <= LANES and 2 * pack * total <= LANES:
        pack *= 2
    part = rows // pack
    wide = -(-n_dev // LANES) * LANES
    anywhere = pl.BlockSpec(memory_space=pl.ANY)
    blocks = (n_dev, part, LANES)
    leg = legendre.transpose(0, 2, 1)
    dma = pltpu.SemaphoreType.DMA
    spec, returned = pl.pallas_call(
        functools.partial(exchange, nb, nf, pack),
        out_shape=(
            jax.ShapeDtypeStruct((1, 2, total, LEV), jnp.bfloat16),
            jax.ShapeDtypeStruct(fourier.shape, jnp.bfloat16),
        ),
        in_specs=[anywhere] * 8,
        out_specs=(anywhere, anywhere),
        scratch_shapes=[
            pltpu.SMEM((n_dev,), jnp.int32),
            pltpu.SMEM((1, wide), jnp.int32),
            pltpu.VMEM((1, n_dev), jnp.int32),
            pltpu.VMEM((1, width), jnp.float32),
            pltpu.VMEM((1, LEV), jnp.float32),
            pltpu.VMEM(leg.shape, jnp.bfloat16),
            pltpu.VMEM((LEV, LEV), jnp.float32),
            pltpu.VMEM((LEV, LEV), jnp.float32),
            pltpu.VMEM(fourier.shape, jnp.bfloat16),
            pltpu.VMEM(blocks, jnp.bfloat16),
            pltpu.VMEM((nb, nf, part, LANES), jnp.bfloat16),
            pltpu.VMEM(blocks, jnp.bfloat16),
            pltpu.VMEM(blocks, jnp.bfloat16),
            pltpu.VMEM((nb, pack * total, LANES), jnp.bfloat16),
            pltpu.VMEM((pack * total, nf * part), jnp.float32),
            pltpu.VMEM((1, wide), jnp.int32),
            pltpu.VMEM((1, 2, total, LEV), jnp.bfloat16),
            pltpu.VMEM(fourier.shape, jnp.bfloat16),
            dma((7,)),
            dma,
            dma((CHUNKS,)),
            dma,
            dma((nb,)),
            dma,
            dma,
        ],
        compiler_params=pltpu.CompilerParams(
            collective_id=0, has_side_effects=True, vmem_limit_bytes=VMEM_LIMIT
        ),
    )(slot_wave, slot_wave[None], quad_weights[None], vert_rates[None], leg, vert_proj, vert_recon, fourier)
    return spec.transpose(0, 1, 3, 2), returned


def solution(mesh):
    placed = (
        P(None, "field", "band"),
        P("band"),
        P(("band", "field"), None, None),
        P(),
        P(),
        P(),
        P(),
    )
    return jax.shard_map(
        per_device,
        mesh=mesh,
        in_specs=placed,
        out_specs=(P(("band", "field"), None, None, None), P(None, "field", "band")),
        check_vma=False,
    )
```

```python
import functools

import jax
import jax.numpy as jnp
from jax import lax
from jax.experimental import pallas as pl
from jax.experimental.pallas import tpu as pltpu
from jax.sharding import PartitionSpec as P

LEV = 96
LANES = 128
UNROLL = 8
UNROLL_PEERS = 7
VMEM_LIMIT = 40 * 1024 * 1024
MESH = pl.DeviceIdType.MESH


def exchange(
    nb, nf, pack, wave_hbm, row_hbm, quad_hbm, rates_hbm, leg_hbm, proj_hbm, recon_hbm, fourier_hbm,
    spec_ref, out_ref,
    wave, order, row, quad, rates, leg, proj, recon, four, send_a, recv_a, send_b, recv_b, table, acc,
    inverse_v,
    small_sem, four_sem, send_a_sem, recv_a_sem, send_b_sem, recv_b_sem,
):
    n_dev = nb * nf
    my_b, my_f = lax.axis_index("band"), lax.axis_index("field")
    me = my_b * nf + my_f
    rows, width = four.shape[1], four.shape[2]
    part = rows // pack
    total = leg.shape[1]

    def wrap(at, size):
        return jnp.where(at >= size, at - size, at)

    fields = [wrap(my_f + step, nf) for step in range(nf)]

    def each_peer(act):
        for f in fields[1:]:
            act(me - my_f + f, (my_b, f))

        @pl.loop(1, nb, unroll=UNROLL_PEERS)
        def _(step):
            b = wrap(my_b + step, nb)
            for f in fields:
                act(b * nf + f, (b, f))

    barrier = pltpu.get_barrier_semaphore()

    def greet(other, where):
        pl.semaphore_signal(barrier, inc=1, device_id=where, device_id_type=MESH)

    each_peer(greet)

    pairs = ((wave_hbm, wave), (quad_hbm, quad), (row_hbm, row), (leg_hbm, leg), (rates_hbm, rates),
             (proj_hbm, proj), (recon_hbm, recon))
    loads = [pltpu.make_async_copy(a, b, small_sem.at[i]) for i, (a, b) in enumerate(pairs)]
    fetch = pltpu.make_async_copy(fourier_hbm, four, four_sem)
    loads[0].start()
    loads[1].start()
    fetch.start()
    for load in loads[2:]:
        load.start()
    loads[0].wait()
    loads[1].wait()
    fetch.wait()

    @pl.loop(0, n_dev, unroll=UNROLL)
    def _(s):
        x = four[jnp.clip(wave[s], 0, n_dev - 1)].astype(jnp.float32) * quad[...]
        pieces = [x[h * part : (h + 1) * part] for h in range(pack)]
        pieces.append(jnp.zeros((part, LANES - pack * width), jnp.float32))
        send_a[s] = jnp.concatenate(pieces, axis=1).astype(jnp.bfloat16)

    pl.semaphore_wait(barrier, n_dev - 1)

    def forward(other, where):
        pltpu.make_async_remote_copy(
            src_ref=send_a.at[other],
            dst_ref=recv_a.at[my_b, my_f],
            send_sem=send_a_sem,
            recv_sem=recv_a_sem.at[my_b],
            device_id=where,
            device_id_type=MESH,
        ).start()

    each_peer(forward)
    pltpu.make_async_copy(send_a.at[me], recv_a.at[my_b, my_f], recv_a_sem.at[my_b]).start()

    loads[2].wait()
    down = lax.broadcasted_iota(jnp.int32, (n_dev, n_dev), 0)
    across = lax.broadcasted_iota(jnp.int32, (n_dev, n_dev), 1)
    aim = lax.broadcasted_iota(jnp.int32, (n_dev, inverse_v.shape[1]), 1)
    source = lax.broadcasted_iota(jnp.int32, (n_dev, inverse_v.shape[1]), 0)
    column = jnp.sum(jnp.where(down == across, row[...].astype(jnp.float32), 0.0), axis=1, keepdims=True)
    hit = column.astype(jnp.int32) == aim
    inverse_v[...] = jnp.sum(jnp.where(hit, source.astype(jnp.float32), 0.0), axis=0, keepdims=True).astype(jnp.int32)

    loads[3].wait()
    for b in range(nb):
        block = leg[0, :, b * width : (b + 1) * width].astype(jnp.float32)
        lines = []
        for h in range(pack):
            line = [jnp.zeros((total, h * width), jnp.float32)] if h else []
            line += [block, jnp.zeros((total, LANES - (h + 1) * width), jnp.float32)]
            lines.append(jnp.concatenate(line, axis=1))
        table[b] = jnp.concatenate(lines, axis=0).astype(jnp.bfloat16)

    to_scalar = pltpu.make_async_copy(inverse_v, order, small_sem.at[2])
    to_scalar.start()
    for load in loads[4:]:
        load.wait()
    degree = lax.broadcasted_iota(jnp.int32, (2 * total, 1), 0)
    degree = jnp.where(degree >= total, degree - total, degree)
    level = degree.astype(jnp.float32)
    gamma = 1.0 / (1.0 + rates[...] * (level * (level + 1.0) / float(total * total)))
    keep = (degree >= wave[me]).astype(jnp.float32)
    to_scalar.wait()

    acc[...] = jnp.zeros_like(acc)

    across_rows = (((1,), (1,)), ((), ()))

    @pl.loop(0, nb)
    def _(step):
        b = wrap(my_b + nb - step, nb)
        pltpu.make_async_copy(recv_a.at[b], recv_a.at[b], recv_a_sem.at[b]).wait()
        data = recv_a[b].reshape(nf * part, LANES)
        acc[...] += lax.dot_general(table[b], data, across_rows, preferred_element_type=jnp.float32)

    per_c = nf * pack // 2
    group = [acc[(g % pack) * total : (g % pack + 1) * total, (g // pack) * part : (g // pack + 1) * part]
             for g in range(nf * pack)]
    direct = jnp.concatenate(
        [jnp.concatenate(group[c * per_c : (c + 1) * per_c], axis=1) for c in range(2)], axis=0
    )
    exact = dict(preferred_element_type=jnp.float32, precision=lax.Precision.HIGHEST)
    modes = lax.dot_general(direct, proj[...], across_rows, **exact) * gamma
    solved = lax.dot_general(modes, recon[...], across_rows, **exact) * keep

    def piece(g):
        c, l = g // per_c, (g % per_c) * part
        return solved[c * total : (c + 1) * total, l : l + part]

    packed = jnp.concatenate(
        [jnp.concatenate([piece(f * pack + h) for f in range(nf)], axis=1) for h in range(pack)], axis=0
    ).T.astype(jnp.bfloat16)

    def synthesize(b):
        got = jnp.dot(packed, table[b], preferred_element_type=jnp.float32)
        send_b[pl.ds(b * nf, nf)] = got.astype(jnp.bfloat16).reshape(nf, part, LANES)

    def backward(b, f):
        other = b * nf + f
        pltpu.make_async_remote_copy(
            src_ref=send_b.at[other],
            dst_ref=recv_b.at[me],
            send_sem=send_b_sem,
            recv_sem=recv_b_sem,
            device_id=(b, f),
            device_id_type=MESH,
        ).start()

    synthesize(wrap(my_b + 1, nb))

    @pl.loop(1, nb, unroll=UNROLL_PEERS)
    def _(step):
        synthesize(wrap(my_b + step + 1, nb))
        for f in fields:
            backward(wrap(my_b + step, nb), f)

    for f in fields[1:]:
        backward(my_b, f)
    pltpu.make_async_copy(send_b.at[me], recv_b.at[me], recv_b_sem).start()
    spec_ref[...] = solved.astype(jnp.bfloat16).reshape(1, 2, total, LEV)
    pltpu.make_async_copy(recv_b, recv_b, recv_b_sem).wait()

    @pl.loop(0, n_dev, unroll=UNROLL)
    def _(w):
        x = recv_b[jnp.clip(order[0, w], 0, n_dev - 1)].astype(jnp.float32)
        for h in range(pack):
            out_ref[w, h * part : (h + 1) * part, :] = x[:, h * width : (h + 1) * width].astype(jnp.bfloat16)

    others = pl.ds(0, n_dev - 1)
    pltpu.make_async_copy(send_a.at[others], send_a.at[others], send_a_sem).wait()
    pltpu.make_async_copy(send_b.at[others], send_b.at[others], send_b_sem).wait()


def per_device(fourier, quad_weights, legendre, slot_wave, vert_proj, vert_recon, vert_rates):
    nb, nf = lax.axis_size("band"), lax.axis_size("field")
    n_dev = nb * nf
    waves, rows, width = fourier.shape
    per_dev, nlat, total = legendre.shape
    assert per_dev == 1 and waves == n_dev and nlat == nb * width and width <= LANES
    pack = 1
    while rows % (2 * pack * 8) == 0 and 2 * pack * width <= LANES and 2 * pack * total <= LANES:
        pack *= 2
    part = rows // pack
    wide = -(-n_dev // LANES) * LANES
    anywhere = pl.BlockSpec(memory_space=pl.ANY)
    blocks = (n_dev, part, LANES)
    leg = legendre.transpose(0, 2, 1)
    dma = pltpu.SemaphoreType.DMA
    spec, returned = pl.pallas_call(
        functools.partial(exchange, nb, nf, pack),
        out_shape=(
            jax.ShapeDtypeStruct((1, 2, total, LEV), jnp.bfloat16),
            jax.ShapeDtypeStruct(fourier.shape, jnp.bfloat16),
        ),
        in_specs=[anywhere] * 8,
        out_specs=(pl.BlockSpec(memory_space=pltpu.VMEM),) * 2,
        scratch_shapes=[
            pltpu.SMEM((n_dev,), jnp.int32),
            pltpu.SMEM((1, wide), jnp.int32),
            pltpu.VMEM((1, n_dev), jnp.int32),
            pltpu.VMEM((1, width), jnp.float32),
            pltpu.VMEM((1, LEV), jnp.float32),
            pltpu.VMEM(leg.shape, jnp.bfloat16),
            pltpu.VMEM((LEV, LEV), jnp.float32),
            pltpu.VMEM((LEV, LEV), jnp.float32),
            pltpu.VMEM(fourier.shape, jnp.bfloat16),
            pltpu.VMEM(blocks, jnp.bfloat16),
            pltpu.VMEM((nb, nf, part, LANES), jnp.bfloat16),
            pltpu.VMEM(blocks, jnp.bfloat16),
            pltpu.VMEM(blocks, jnp.bfloat16),
            pltpu.VMEM((nb, pack * total, LANES), jnp.bfloat16),
            pltpu.VMEM((pack * total, nf * part), jnp.float32),
            pltpu.VMEM((1, wide), jnp.int32),
            dma((7,)),
            dma,
            dma,
            dma((nb,)),
            dma,
            dma,
        ],
        compiler_params=pltpu.CompilerParams(
            collective_id=0, has_side_effects=True, vmem_limit_bytes=VMEM_LIMIT
        ),
    )(*[pltpu.with_memory_space_constraint(a, pltpu.HBM) for a in (slot_wave, slot_wave[None], quad_weights[None], vert_rates[None], leg, vert_proj, vert_recon, fourier)])
    return spec.transpose(0, 1, 3, 2), returned


def solution(mesh):
    placed = (
        P(None, "field", "band"),
        P("band"),
        P(("band", "field"), None, None),
        P(),
        P(),
        P(),
        P(),
    )
    return jax.shard_map(
        per_device,
        mesh=mesh,
        in_specs=placed,
        out_specs=(P(("band", "field"), None, None, None), P(None, "field", "band")),
        check_vma=False,
    )
```

```python
import functools

import jax
import jax.numpy as jnp
from jax import lax
from jax.experimental import pallas as pl
from jax.experimental.pallas import tpu as pltpu
from jax.sharding import PartitionSpec as P

LEV = 96
LANES = 128
UNROLL = 8
UNROLL_PEERS = 7
VMEM_LIMIT = 40 * 1024 * 1024
MESH = pl.DeviceIdType.MESH


def exchange(
    nb, nf, pack, wave_hbm, row_hbm, quad_hbm, rates_hbm, leg_hbm, proj_hbm, recon_hbm, fourier_hbm,
    spec_ref, out_ref,
    wave, order, row, quad, rates, leg, proj, recon, four, send_a, recv_a, send_b, recv_b, table, acc,
    inverse_v,
    small_sem, four_sem, send_a_sem, recv_a_sem, send_b_sem, recv_b_sem,
):
    n_dev = nb * nf
    my_b, my_f = lax.axis_index("band"), lax.axis_index("field")
    me = my_b * nf + my_f
    rows, width = four.shape[1], four.shape[2]
    part = rows // pack
    total = leg.shape[1]

    def wrap(at, size):
        return jnp.where(at >= size, at - size, at)

    fields = [wrap(my_f + step, nf) for step in range(nf)]

    def each_peer(act):
        for f in fields[1:]:
            act(me - my_f + f, (my_b, f))

        @pl.loop(1, nb, unroll=UNROLL_PEERS)
        def _(step):
            b = lax.rem(my_b + nb - step, nb)
            for f in fields:
                act(b * nf + f, (b, f))

    barrier = pltpu.get_barrier_semaphore()

    def greet(other, where):
        pl.semaphore_signal(barrier, inc=1, device_id=where, device_id_type=MESH)

    each_peer(greet)

    pairs = ((wave_hbm, wave), (quad_hbm, quad), (row_hbm, row), (leg_hbm, leg), (rates_hbm, rates),
             (proj_hbm, proj), (recon_hbm, recon))
    loads = [pltpu.make_async_copy(a, b, small_sem.at[i]) for i, (a, b) in enumerate(pairs)]
    fetch = pltpu.make_async_copy(fourier_hbm, four, four_sem)
    loads[0].start()
    loads[1].start()
    fetch.start()
    for load in loads[2:]:
        load.start()
    loads[0].wait()
    loads[1].wait()
    fetch.wait()

    @pl.loop(0, n_dev, unroll=UNROLL)
    def _(s):
        x = four[jnp.clip(wave[s], 0, n_dev - 1)].astype(jnp.float32) * quad[...]
        pieces = [x[h * part : (h + 1) * part] for h in range(pack)]
        pieces.append(jnp.zeros((part, LANES - pack * width), jnp.float32))
        send_a[s] = jnp.concatenate(pieces, axis=1).astype(jnp.bfloat16)

    pl.semaphore_wait(barrier, n_dev - 1)

    def forward(other, where):
        pltpu.make_async_remote_copy(
            src_ref=send_a.at[other],
            dst_ref=recv_a.at[my_b, my_f],
            send_sem=send_a_sem,
            recv_sem=recv_a_sem.at[my_b],
            device_id=where,
            device_id_type=MESH,
        ).start()

    each_peer(forward)
    pltpu.make_async_copy(send_a.at[me], recv_a.at[my_b, my_f], recv_a_sem.at[my_b]).start()

    loads[2].wait()
    down = lax.broadcasted_iota(jnp.int32, (n_dev, n_dev), 0)
    across = lax.broadcasted_iota(jnp.int32, (n_dev, n_dev), 1)
    aim = lax.broadcasted_iota(jnp.int32, (n_dev, inverse_v.shape[1]), 1)
    source = lax.broadcasted_iota(jnp.int32, (n_dev, inverse_v.shape[1]), 0)
    column = jnp.sum(jnp.where(down == across, row[...].astype(jnp.float32), 0.0), axis=1, keepdims=True)
    hit = column.astype(jnp.int32) == aim
    inverse_v[...] = jnp.sum(jnp.where(hit, source.astype(jnp.float32), 0.0), axis=0, keepdims=True).astype(jnp.int32)

    loads[3].wait()
    for b in range(nb):
        block = leg[0, :, b * width : (b + 1) * width].astype(jnp.float32)
        lines = []
        for h in range(pack):
            line = [jnp.zeros((total, h * width), jnp.float32)] if h else []
            line += [block, jnp.zeros((total, LANES - (h + 1) * width), jnp.float32)]
            lines.append(jnp.concatenate(line, axis=1))
        table[b] = jnp.concatenate(lines, axis=0).astype(jnp.bfloat16)

    to_scalar = pltpu.make_async_copy(inverse_v, order, small_sem.at[2])
    to_scalar.start()
    for load in loads[4:]:
        load.wait()
    degree = lax.broadcasted_iota(jnp.int32, (2 * total, 1), 0)
    degree = jnp.where(degree >= total, degree - total, degree)
    level = degree.astype(jnp.float32)
    gamma = 1.0 / (1.0 + rates[...] * (level * (level + 1.0) / float(total * total)))
    keep = (degree >= wave[me]).astype(jnp.float32)
    to_scalar.wait()

    acc[...] = jnp.zeros_like(acc)

    across_rows = (((1,), (1,)), ((), ()))

    @pl.loop(0, nb)
    def _(step):
        b = wrap(my_b + step, nb)
        pltpu.make_async_copy(recv_a.at[b], recv_a.at[b], recv_a_sem.at[b]).wait()
        data = recv_a[b].reshape(nf * part, LANES)
        acc[...] += lax.dot_general(table[b], data, across_rows, preferred_element_type=jnp.float32)

    per_c = nf * pack // 2
    group = [acc[(g % pack) * total : (g % pack + 1) * total, (g // pack) * part : (g // pack + 1) * part]
             for g in range(nf * pack)]
    direct = jnp.concatenate(
        [jnp.concatenate(group[c * per_c : (c + 1) * per_c], axis=1) for c in range(2)], axis=0
    )
    exact = dict(preferred_element_type=jnp.float32, precision=lax.Precision.HIGHEST)
    modes = lax.dot_general(direct, proj[...], across_rows, **exact) * gamma
    solved = lax.dot_general(modes, recon[...], across_rows, **exact) * keep

    def piece(g):
        c, l = g // per_c, (g % per_c) * part
        return solved[c * total : (c + 1) * total, l : l + part]

    packed = jnp.concatenate(
        [jnp.concatenate([piece(f * pack + h) for f in range(nf)], axis=1) for h in range(pack)], axis=0
    ).T.astype(jnp.bfloat16)

    def synthesize(b):
        got = jnp.dot(packed, table[b], preferred_element_type=jnp.float32)
        send_b[pl.ds(b * nf, nf)] = got.astype(jnp.bfloat16).reshape(nf, part, LANES)

    def backward(b, f):
        other = b * nf + f
        pltpu.make_async_remote_copy(
            src_ref=send_b.at[other],
            dst_ref=recv_b.at[me],
            send_sem=send_b_sem,
            recv_sem=recv_b_sem,
            device_id=(b, f),
            device_id_type=MESH,
        ).start()

    synthesize(lax.rem(my_b + nb - 1, nb))

    @pl.loop(1, nb, unroll=UNROLL_PEERS)
    def _(step):
        synthesize(lax.rem(my_b + nb + nb - step - 1, nb))
        for f in fields:
            backward(lax.rem(my_b + nb - step, nb), f)

    for f in fields[1:]:
        backward(my_b, f)
    pltpu.make_async_copy(send_b.at[me], recv_b.at[me], recv_b_sem).start()
    spec_ref[...] = solved.astype(jnp.bfloat16).reshape(1, 2, total, LEV)
    pltpu.make_async_copy(recv_b, recv_b, recv_b_sem).wait()

    @pl.loop(0, n_dev, unroll=UNROLL)
    def _(w):
        x = recv_b[jnp.clip(order[0, w], 0, n_dev - 1)].astype(jnp.float32)
        for h in range(pack):
            out_ref[w, h * part : (h + 1) * part, :] = x[:, h * width : (h + 1) * width].astype(jnp.bfloat16)

    others = pl.ds(0, n_dev - 1)
    pltpu.make_async_copy(send_a.at[others], send_a.at[others], send_a_sem).wait()
    pltpu.make_async_copy(send_b.at[others], send_b.at[others], send_b_sem).wait()


def hand_over(spec_in, grid_in, spec_out, grid_out, sems):
    copies = [
        pltpu.make_async_copy(grid_in, grid_out, sems.at[0]),
        pltpu.make_async_copy(spec_in, spec_out, sems.at[1]),
    ]
    for copy in copies:
        copy.start()
    for copy in copies:
        copy.wait()


def per_device(fourier, quad_weights, legendre, slot_wave, vert_proj, vert_recon, vert_rates):
    nb, nf = lax.axis_size("band"), lax.axis_size("field")
    n_dev = nb * nf
    waves, rows, width = fourier.shape
    per_dev, nlat, total = legendre.shape
    assert per_dev == 1 and waves == n_dev and nlat == nb * width and width <= LANES
    pack = 1
    while rows % (2 * pack * 8) == 0 and 2 * pack * width <= LANES and 2 * pack * total <= LANES:
        pack *= 2
    part = rows // pack
    wide = -(-n_dev // LANES) * LANES
    anywhere = pl.BlockSpec(memory_space=pl.ANY)
    blocks = (n_dev, part, LANES)
    leg = legendre.transpose(0, 2, 1)
    dma = pltpu.SemaphoreType.DMA
    spec, returned = pl.pallas_call(
        functools.partial(exchange, nb, nf, pack),
        out_shape=(
            jax.ShapeDtypeStruct((1, 2, total, LEV), jnp.bfloat16),
            jax.ShapeDtypeStruct(fourier.shape, jnp.bfloat16),
        ),
        in_specs=[anywhere] * 8,
        out_specs=(pl.BlockSpec(memory_space=pltpu.VMEM),) * 2,
        scratch_shapes=[
            pltpu.SMEM((n_dev,), jnp.int32),
            pltpu.SMEM((1, wide), jnp.int32),
            pltpu.VMEM((1, n_dev), jnp.int32),
            pltpu.VMEM((1, width), jnp.float32),
            pltpu.VMEM((1, LEV), jnp.float32),
            pltpu.VMEM(leg.shape, jnp.bfloat16),
            pltpu.VMEM((LEV, LEV), jnp.float32),
            pltpu.VMEM((LEV, LEV), jnp.float32),
            pltpu.VMEM(fourier.shape, jnp.bfloat16),
            pltpu.VMEM(blocks, jnp.bfloat16),
            pltpu.VMEM((nb, nf, part, LANES), jnp.bfloat16),
            pltpu.VMEM(blocks, jnp.bfloat16),
            pltpu.VMEM(blocks, jnp.bfloat16),
            pltpu.VMEM((nb, pack * total, LANES), jnp.bfloat16),
            pltpu.VMEM((pack * total, nf * part), jnp.float32),
            pltpu.VMEM((1, wide), jnp.int32),
            dma((7,)),
            dma,
            dma,
            dma((nb,)),
            dma,
            dma,
        ],
        compiler_params=pltpu.CompilerParams(
            collective_id=0, has_side_effects=True, vmem_limit_bytes=VMEM_LIMIT
        ),
    )(*[pltpu.with_memory_space_constraint(a, pltpu.HBM) for a in (slot_wave, slot_wave[None], quad_weights[None], vert_rates[None], leg, vert_proj, vert_recon, fourier)])
    spec, returned = pl.pallas_call(
        hand_over,
        out_shape=(
            jax.ShapeDtypeStruct(spec.shape, spec.dtype),
            jax.ShapeDtypeStruct(returned.shape, returned.dtype),
        ),
        in_specs=[anywhere] * 2,
        out_specs=(anywhere, anywhere),
        scratch_shapes=[dma((2,))],
        compiler_params=pltpu.CompilerParams(vmem_limit_bytes=VMEM_LIMIT),
    )(spec, returned)
    return spec.transpose(0, 1, 3, 2), returned


def solution(mesh):
    placed = (
        P(None, "field", "band"),
        P("band"),
        P(("band", "field"), None, None),
        P(),
        P(),
        P(),
        P(),
    )
    return jax.shard_map(
        per_device,
        mesh=mesh,
        in_specs=placed,
        out_specs=(P(("band", "field"), None, None, None), P(None, "field", "band")),
        check_vma=False,
    )
```

```python
import functools

import jax
import jax.numpy as jnp
from jax import lax
from jax.experimental import pallas as pl
from jax.experimental.pallas import tpu as pltpu
from jax.sharding import PartitionSpec as P

LEV = 96
LANES = 128
UNROLL = 16
UNROLL_PEERS = 7
VMEM_LIMIT = 40 * 1024 * 1024
MESH = pl.DeviceIdType.MESH


def exchange(
    nb, nf, pack, wave_hbm, row_hbm, quad_hbm, rates_hbm, leg_hbm, proj_hbm, recon_hbm, fourier_hbm,
    spec_ref, out_ref,
    wave, order, row, quad, rates, leg, proj, recon, four, send_a, recv_a, send_b, recv_b, table, acc,
    inverse_v,
    small_sem, four_sem, send_a_sem, recv_a_sem, send_b_sem, recv_b_sem,
):
    n_dev = nb * nf
    my_b, my_f = lax.axis_index("band"), lax.axis_index("field")
    me = my_b * nf + my_f
    rows, width = four.shape[1], four.shape[2]
    part = rows // pack
    total = leg.shape[1]

    def wrap(at, size):
        return jnp.where(at >= size, at - size, at)

    fields = [wrap(my_f + step, nf) for step in range(nf)]

    def each_peer(act):
        for f in fields[1:]:
            act(me - my_f + f, (my_b, f))

        @pl.loop(1, nb, unroll=UNROLL_PEERS)
        def _(step):
            b = lax.rem(my_b + nb - step, nb)
            for f in fields:
                act(b * nf + f, (b, f))

    barrier = pltpu.get_barrier_semaphore()

    def greet(other, where):
        pl.semaphore_signal(barrier, inc=1, device_id=where, device_id_type=MESH)

    each_peer(greet)

    pairs = ((wave_hbm, wave), (quad_hbm, quad), (row_hbm, row), (leg_hbm, leg), (rates_hbm, rates),
             (proj_hbm, proj), (recon_hbm, recon))
    loads = [pltpu.make_async_copy(a, b, small_sem.at[i]) for i, (a, b) in enumerate(pairs)]
    fetch = pltpu.make_async_copy(fourier_hbm, four, four_sem)
    loads[0].start()
    loads[1].start()
    fetch.start()
    for load in loads[2:]:
        load.start()
    loads[0].wait()
    loads[1].wait()
    fetch.wait()

    @pl.loop(0, n_dev, unroll=UNROLL)
    def _(s):
        x = four[jnp.clip(wave[s], 0, n_dev - 1)].astype(jnp.float32) * quad[...]
        pieces = [x[h * part : (h + 1) * part] for h in range(pack)]
        pieces.append(jnp.zeros((part, LANES - pack * width), jnp.float32))
        send_a[s] = jnp.concatenate(pieces, axis=1).astype(jnp.bfloat16)

    pl.semaphore_wait(barrier, n_dev - 1)

    def forward(other, where):
        pltpu.make_async_remote_copy(
            src_ref=send_a.at[other],
            dst_ref=recv_a.at[my_b, my_f],
            send_sem=send_a_sem,
            recv_sem=recv_a_sem.at[my_b],
            device_id=where,
            device_id_type=MESH,
        ).start()

    each_peer(forward)
    pltpu.make_async_copy(send_a.at[me], recv_a.at[my_b, my_f], recv_a_sem.at[my_b]).start()

    loads[2].wait()
    down = lax.broadcasted_iota(jnp.int32, (n_dev, n_dev), 0)
    across = lax.broadcasted_iota(jnp.int32, (n_dev, n_dev), 1)
    aim = lax.broadcasted_iota(jnp.int32, (n_dev, inverse_v.shape[1]), 1)
    source = lax.broadcasted_iota(jnp.int32, (n_dev, inverse_v.shape[1]), 0)
    column = jnp.sum(jnp.where(down == across, row[...].astype(jnp.float32), 0.0), axis=1, keepdims=True)
    hit = column.astype(jnp.int32) == aim
    inverse_v[...] = jnp.sum(jnp.where(hit, source.astype(jnp.float32), 0.0), axis=0, keepdims=True).astype(jnp.int32)

    loads[3].wait()
    for b in range(nb):
        block = leg[0, :, b * width : (b + 1) * width].astype(jnp.float32)
        lines = []
        for h in range(pack):
            line = [jnp.zeros((total, h * width), jnp.float32)] if h else []
            line += [block, jnp.zeros((total, LANES - (h + 1) * width), jnp.float32)]
            lines.append(jnp.concatenate(line, axis=1))
        table[b] = jnp.concatenate(lines, axis=0).astype(jnp.bfloat16)

    to_scalar = pltpu.make_async_copy(inverse_v, order, small_sem.at[2])
    to_scalar.start()
    for load in loads[4:]:
        load.wait()
    degree = lax.broadcasted_iota(jnp.int32, (2 * total, 1), 0)
    degree = jnp.where(degree >= total, degree - total, degree)
    level = degree.astype(jnp.float32)
    gamma = 1.0 / (1.0 + rates[...] * (level * (level + 1.0) / float(total * total)))
    keep = (degree >= wave[me]).astype(jnp.float32)
    to_scalar.wait()

    acc[...] = jnp.zeros_like(acc)

    across_rows = (((1,), (1,)), ((), ()))

    @pl.loop(0, nb)
    def _(step):
        b = wrap(my_b + step, nb)
        pltpu.make_async_copy(recv_a.at[b], recv_a.at[b], recv_a_sem.at[b]).wait()
        data = recv_a[b].reshape(nf * part, LANES)
        acc[...] += lax.dot_general(table[b], data, across_rows, preferred_element_type=jnp.float32)

    per_c = nf * pack // 2
    group = [acc[(g % pack) * total : (g % pack + 1) * total, (g // pack) * part : (g // pack + 1) * part]
             for g in range(nf * pack)]
    direct = jnp.concatenate(
        [jnp.concatenate(group[c * per_c : (c + 1) * per_c], axis=1) for c in range(2)], axis=0
    )
    exact = dict(preferred_element_type=jnp.float32, precision=lax.Precision.HIGHEST)
    modes = lax.dot_general(direct, proj[...], across_rows, **exact) * gamma
    solved = lax.dot_general(modes, recon[...], across_rows, **exact) * keep

    def piece(g):
        c, l = g // per_c, (g % per_c) * part
        return solved[c * total : (c + 1) * total, l : l + part]

    packed = jnp.concatenate(
        [jnp.concatenate([piece(f * pack + h) for f in range(nf)], axis=1) for h in range(pack)], axis=0
    ).T.astype(jnp.bfloat16)

    def synthesize(b):
        got = jnp.dot(packed, table[b], preferred_element_type=jnp.float32)
        send_b[pl.ds(b * nf, nf)] = got.astype(jnp.bfloat16).reshape(nf, part, LANES)

    def backward(b, f):
        other = b * nf + f
        pltpu.make_async_remote_copy(
            src_ref=send_b.at[other],
            dst_ref=recv_b.at[me],
            send_sem=send_b_sem,
            recv_sem=recv_b_sem,
            device_id=(b, f),
            device_id_type=MESH,
        ).start()

    synthesize(lax.rem(my_b + nb - 1, nb))

    @pl.loop(1, nb, unroll=UNROLL_PEERS)
    def _(step):
        synthesize(lax.rem(my_b + nb + nb - step - 1, nb))
        for f in fields:
            backward(lax.rem(my_b + nb - step, nb), f)

    for f in fields[1:]:
        backward(my_b, f)
    pltpu.make_async_copy(send_b.at[me], recv_b.at[me], recv_b_sem).start()
    spec_ref[...] = solved.astype(jnp.bfloat16).reshape(1, 2, total, LEV)
    pltpu.make_async_copy(recv_b, recv_b, recv_b_sem).wait()

    @pl.loop(0, n_dev, unroll=UNROLL)
    def _(w):
        x = recv_b[jnp.clip(order[0, w], 0, n_dev - 1)].astype(jnp.float32)
        for h in range(pack):
            out_ref[w, h * part : (h + 1) * part, :] = x[:, h * width : (h + 1) * width].astype(jnp.bfloat16)

    others = pl.ds(0, n_dev - 1)
    pltpu.make_async_copy(send_a.at[others], send_a.at[others], send_a_sem).wait()
    pltpu.make_async_copy(send_b.at[others], send_b.at[others], send_b_sem).wait()


def hand_over(spec_in, grid_in, spec_out, grid_out, sems):
    copies = [
        pltpu.make_async_copy(grid_in, grid_out, sems.at[0]),
        pltpu.make_async_copy(spec_in, spec_out, sems.at[1]),
    ]
    for copy in copies:
        copy.start()
    for copy in copies:
        copy.wait()


def per_device(fourier, quad_weights, legendre, slot_wave, vert_proj, vert_recon, vert_rates):
    nb, nf = lax.axis_size("band"), lax.axis_size("field")
    n_dev = nb * nf
    waves, rows, width = fourier.shape
    per_dev, nlat, total = legendre.shape
    assert per_dev == 1 and waves == n_dev and nlat == nb * width and width <= LANES
    pack = 1
    while rows % (2 * pack * 8) == 0 and 2 * pack * width <= LANES and 2 * pack * total <= LANES:
        pack *= 2
    part = rows // pack
    wide = -(-n_dev // LANES) * LANES
    anywhere = pl.BlockSpec(memory_space=pl.ANY)
    blocks = (n_dev, part, LANES)
    leg = legendre.transpose(0, 2, 1)
    dma = pltpu.SemaphoreType.DMA
    spec, returned = pl.pallas_call(
        functools.partial(exchange, nb, nf, pack),
        out_shape=(
            jax.ShapeDtypeStruct((1, 2, total, LEV), jnp.bfloat16),
            jax.ShapeDtypeStruct(fourier.shape, jnp.bfloat16),
        ),
        in_specs=[anywhere] * 8,
        out_specs=(pl.BlockSpec(memory_space=pltpu.VMEM),) * 2,
        scratch_shapes=[
            pltpu.SMEM((n_dev,), jnp.int32),
            pltpu.SMEM((1, wide), jnp.int32),
            pltpu.VMEM((1, n_dev), jnp.int32),
            pltpu.VMEM((1, width), jnp.float32),
            pltpu.VMEM((1, LEV), jnp.float32),
            pltpu.VMEM(leg.shape, jnp.bfloat16),
            pltpu.VMEM((LEV, LEV), jnp.float32),
            pltpu.VMEM((LEV, LEV), jnp.float32),
            pltpu.VMEM(fourier.shape, jnp.bfloat16),
            pltpu.VMEM(blocks, jnp.bfloat16),
            pltpu.VMEM((nb, nf, part, LANES), jnp.bfloat16),
            pltpu.VMEM(blocks, jnp.bfloat16),
            pltpu.VMEM(blocks, jnp.bfloat16),
            pltpu.VMEM((nb, pack * total, LANES), jnp.bfloat16),
            pltpu.VMEM((pack * total, nf * part), jnp.float32),
            pltpu.VMEM((1, wide), jnp.int32),
            dma((7,)),
            dma,
            dma,
            dma((nb,)),
            dma,
            dma,
        ],
        compiler_params=pltpu.CompilerParams(
            collective_id=0, has_side_effects=True, vmem_limit_bytes=VMEM_LIMIT
        ),
    )(*[pltpu.with_memory_space_constraint(a, pltpu.HBM) for a in (slot_wave, slot_wave[None], quad_weights[None], vert_rates[None], leg, vert_proj, vert_recon, fourier)])
    spec, returned = pl.pallas_call(
        hand_over,
        out_shape=(
            jax.ShapeDtypeStruct(spec.shape, spec.dtype),
            jax.ShapeDtypeStruct(returned.shape, returned.dtype),
        ),
        in_specs=[anywhere] * 2,
        out_specs=(anywhere, anywhere),
        scratch_shapes=[dma((2,))],
        compiler_params=pltpu.CompilerParams(vmem_limit_bytes=VMEM_LIMIT),
    )(spec, returned)
    return spec.transpose(0, 1, 3, 2), returned


def solution(mesh):
    placed = (
        P(None, "field", "band"),
        P("band"),
        P(("band", "field"), None, None),
        P(),
        P(),
        P(),
        P(),
    )
    return jax.shard_map(
        per_device,
        mesh=mesh,
        in_specs=placed,
        out_specs=(P(("band", "field"), None, None, None), P(None, "field", "band")),
        check_vma=False,
    )
```
